32 devices in a mesh: req: 4 (over y, z), cp: 8 (over x, core).
Axes of the slice: x: 4, y: 2, z: 2, core: 2. Of those that a mesh axis runs over, the one named last changes fastest.
The devices are a block of a 4x4x8 slice.
Arguments:
- x: bfloat16 [16384, 2048], P(('req', 'cp')), parts along dimension 0
- pos: int32 [16384], P(('req', 'cp')), parts along dimension 0
- g1: bfloat16 [2, 2048], replicated
- g2: bfloat16 [2, 2048], replicated
- wq: bfloat16 [2, 2048, 2048], replicated
- wk: bfloat16 [2, 2048, 2048], replicated
- wv: bfloat16 [2, 2048, 2048], replicated
- wo: bfloat16 [2, 2048, 2048], replicated
- w1: bfloat16 [2, 2048, 8192], replicated
- w3: bfloat16 [2, 2048, 8192], replicated
- w2: bfloat16 [2, 8192, 2048], replicated
Outputs:
- output 1: bfloat16 [16384, 2048], P(('req', 'cp')), parts along dimension 0
- output 2: bfloat16 [2, 16384, 16, 128], P(None, 'req', 'cp'), parts along dimension 1
- output 3: bfloat16 [2, 16384, 16, 128], P(None, 'req', 'cp'), parts along dimension 1
There are 4 independent parts. The reference program is written for one: setup_inputs(seed, part) draws one part's arguments, and reference() takes and returns one part's arrays. A program takes and returns all parts, laid end to end along the dimension named above; an argument that names none is the same for every part.
All inputs are finite; a program needn't handle non-finite values.
Results may differ from the reference program's by a relative error of at most 0.018145.
Values are sent between devices in bfloat16 or wider.
A program may use at most 768 MiB of HBM per device.

```python
import jax
import jax.numpy as jnp
from jax import lax
import numpy as np

D = 2048
HEADS = 16
HEAD = 128
FF = 8192
LAYERS = 2
S_DEV = 512
CP = 8

SEQ = CP * S_DEV
SEG = S_DEV // 2


def _layout():
    rows = [np.arange(c * SEG, (c + 1) * SEG) for i in range(CP) for c in (i, 2 * CP - 1 - i)]
    return np.concatenate(rows).astype(np.int32)


def setup_inputs(seed: int = 0, part: int = 0) -> dict:
    key = jax.random.PRNGKey(seed)
    kx, ko = jax.random.split(jax.random.fold_in(key, part))
    ks = jax.random.split(key, 9)
    hd = HEADS * HEAD

    def w(k, shape, scale):
        return (jax.random.normal(k, shape, jnp.float32) * scale).astype(jnp.bfloat16)

    def gain(k):
        return (1.0 + 0.2 * jax.random.normal(k, (LAYERS, D), jnp.float32)).astype(jnp.bfloat16)

    p0 = jax.random.randint(ko, (), 0, 4096, jnp.int32)
    return {
        "x": jax.random.normal(kx, (SEQ, D), jnp.float32).astype(jnp.bfloat16),
        "pos": p0 + jnp.asarray(_layout()),
        "g1": gain(ks[0]),
        "g2": gain(ks[1]),
        "wq": w(ks[2], (LAYERS, D, hd), 1.7 * D ** -0.5),
        "wk": w(ks[3], (LAYERS, D, hd), 1.7 * D ** -0.5),
        "wv": w(ks[4], (LAYERS, D, hd), D ** -0.5),
        "wo": w(ks[5], (LAYERS, hd, D), hd ** -0.5),
        "w1": w(ks[6], (LAYERS, D, FF), D ** -0.5),
        "w3": w(ks[7], (LAYERS, D, FF), D ** -0.5),
        "w2": w(ks[8], (LAYERS, FF, D), FF ** -0.5),
    }


def _norm(x, g):
    x32 = x.astype(jnp.float32)
    r = lax.rsqrt(jnp.mean(x32 * x32, axis=-1, keepdims=True) + 1e-5)
    return (x32 * r * g.astype(jnp.float32)).astype(jnp.bfloat16)


def _rope(t, pos):
    half = HEAD // 2
    inv = 1.0 / (10000.0 ** (jnp.arange(half, dtype=jnp.float32) * (2.0 / HEAD)))
    ang = pos.astype(jnp.float32)[:, None] * inv[None, :]
    c = jnp.cos(ang)[:, None, :]
    s = jnp.sin(ang)[:, None, :]
    t1, t2 = t[..., :half], t[..., half:]
    return jnp.concatenate([t1 * c - t2 * s, t2 * c + t1 * s], axis=-1)


def _attention(q, k, v, pos):
    nb = SEQ // SEG
    scale = HEAD ** -0.5

    def head(a):
        qh, kh, vh = a

        def blk(b):
            qb, pb = b
            s = jnp.dot(qb, kh.T, preferred_element_type=jnp.float32) * scale
            s = jnp.where(pos[None, :] <= pb[:, None], s, -jnp.inf)
            p = jax.nn.softmax(s, axis=-1).astype(jnp.bfloat16)
            return jnp.dot(p, vh, preferred_element_type=jnp.float32).astype(jnp.bfloat16)

        o = lax.map(blk, (qh.reshape(nb, SEG, HEAD), pos.reshape(nb, SEG)))
        return o.reshape(SEQ, HEAD)

    o = lax.map(head, (q.transpose(1, 0, 2), k.transpose(1, 0, 2), v.transpose(1, 0, 2)))
    return o.transpose(1, 0, 2).reshape(SEQ, HEADS * HEAD)


def reference(x, pos, g1, g2, wq, wk, wv, wo, w1, w3, w2):
    order = jnp.argsort(pos)

    def layer(x, w):
        a1, a2, bq, bk, bv, bo, b1, b3, b2 = w
        h = _norm(x, a1)
        q = _rope(jnp.dot(h, bq, preferred_element_type=jnp.float32).reshape(SEQ, HEADS, HEAD), pos).astype(jnp.bfloat16)
        k = _rope(jnp.dot(h, bk, preferred_element_type=jnp.float32).reshape(SEQ, HEADS, HEAD), pos).astype(jnp.bfloat16)
        v = jnp.dot(h, bv, preferred_element_type=jnp.float32).astype(jnp.bfloat16).reshape(SEQ, HEADS, HEAD)
        o = _attention(q, k, v, pos)
        x = (x.astype(jnp.float32) + jnp.dot(o, bo, preferred_element_type=jnp.float32)).astype(jnp.bfloat16)
        h2 = _norm(x, a2)
        u = (jax.nn.silu(jnp.dot(h2, b1, preferred_element_type=jnp.float32))
             * jnp.dot(h2, b3, preferred_element_type=jnp.float32)).astype(jnp.bfloat16)
        x = (x.astype(jnp.float32) + jnp.dot(u, b2, preferred_element_type=jnp.float32)).astype(jnp.bfloat16)
        return x, (k[order], v[order])

    y, (kc, vc) = lax.scan(layer, x, (g1, g2, wq, wk, wv, wo, w1, w3, w2))
    return y, kc, vc
```

```python
import functools
import math

import jax
import jax.numpy as jnp
from jax import lax
from jax.experimental import pallas as pl
from jax.experimental.pallas import tpu as pltpu
from jax.sharding import PartitionSpec as P

HEAD = 128
TILE = 512
NBUF = 8
F32 = jnp.float32
BF16 = jnp.bfloat16
VMEM_LIMIT = 60 * 1024 * 1024


def _tables(pos):
    half = HEAD // 2
    inv = 1.0 / (10000.0 ** (jnp.arange(half, dtype=F32) * (2.0 / HEAD)))
    ang = pos.astype(F32)[:, None] * inv
    c, s = jnp.cos(ang), jnp.sin(ang)
    return jnp.concatenate([c, c], axis=1), jnp.concatenate([-s, s], axis=1)


def _norm_to(dst, x, g):
    x32 = x.astype(F32)
    r = lax.rsqrt(jnp.mean(x32 * x32, axis=-1, keepdims=True) + 1e-5)
    dst[...] = (x32 * r * g.astype(F32)).astype(BF16)


def _dense_kernel(layer, mlp, qkv, *refs):
    refs = list(refs)
    x_ref = refs.pop(0)
    if mlp:
        o_ref, g2_ref, wo, w1, w3, w2 = refs[:6]
        refs = refs[6:]
    if qkv:
        g1_ref, cos_ref, sin_ref, wq, wk, wv = refs[:6]
        refs = refs[6:]
    if mlp:
        y_ref = refs.pop(0)
    if qkv:
        qkv_ref = refs.pop(0)
    h_s, wbuf, sems = refs[:3]
    if mlp:
        xm_s, u_s = refs[3:5]
    rows, d = x_ref.shape
    nk = wbuf.shape[1]

    segs = []
    base = 0
    if mlp:
        no, nf = wo.shape[2] // TILE, w1.shape[2] // TILE
        kk = w2.shape[1] // nk
        ny = w2.shape[2] // TILE
        b_o, b_1, b_2 = 0, no, no + 2 * nf
        segs.append((b_o, no, lambda i: [(None, wo.at[layer, :, pl.ds(i * TILE, TILE)])]))
        segs.append((b_1, 2 * nf, lambda i: [(0, w1.at[layer, :, pl.ds((i // 2) * TILE, TILE)]),
                                             (1, w3.at[layer, :, pl.ds((i // 2) * TILE, TILE)])]))
        segs.append((b_2, ny * kk, lambda i: [(None, w2.at[layer, pl.ds((i % kk) * nk, nk),
                                                          pl.ds((i // kk) * TILE, TILE)])]))
        base = b_2 + ny * kk
    if qkv:
        lq = layer + 1
        nq = wq.shape[2] // TILE
        b_q = base
        segs.append((b_q, 3 * nq, lambda i: [(0, wq.at[lq, :, pl.ds((i // 3) * TILE, TILE)]),
                                             (1, wk.at[lq, :, pl.ds((i // 3) * TILE, TILE)]),
                                             (2, wv.at[lq, :, pl.ds((i // 3) * TILE, TILE)])]))
        base = b_q + 3 * nq
    total = base

    def start(t):
        slot = lax.rem(t, NBUF) if not isinstance(t, int) else t % NBUF
        for b, n, srcs in segs:
            if isinstance(t, int):
                if b <= t < b + n:
                    lst = srcs(t - b)
                    src = lst[(t - b) % len(lst)][1]
                    pltpu.make_async_copy(src, wbuf.at[slot], sems.at[slot]).start()
                continue
            i = t - b
            lst = srcs(i)
            for which, src in lst:
                cond = (t >= b) & (t < b + n)
                if which is not None:
                    cond = cond & (lax.rem(i, len(lst)) == which)

                @pl.when(cond)
                def _(src=src):
                    pltpu.make_async_copy(src, wbuf.at[slot], sems.at[slot]).start()

    any_src = segs[0][2](0)[0][1]

    def ready(t):
        slot = lax.rem(t, NBUF)
        pltpu.make_async_copy(any_src, wbuf.at[slot], sems.at[slot]).wait()
        return slot

    for t in range(min(NBUF, total)):
        start(t)

    if mlp:
        for j in range(o_ref.shape[0]):
            w = o_ref.shape[2]
            h_s[:, j * w:(j + 1) * w] = o_ref[j]

        @pl.loop(0, no)
        def _(i):
            t = b_o + i
            slot = ready(t)
            col = pl.ds(pl.multiple_of(i * TILE, TILE), TILE)
            r = jnp.dot(h_s[...], wbuf[slot], preferred_element_type=F32)
            xm_s[:, col] = (x_ref[:, col].astype(F32) + r).astype(BF16)
            start(t + NBUF)

        _norm_to(h_s, xm_s[...], g2_ref[...])

        @pl.loop(0, nf)
        def _(i):
            t = b_1 + 2 * i
            s1 = ready(t)
            s3 = ready(t + 1)
            a = jnp.dot(h_s[...], wbuf[s1], preferred_element_type=F32)
            b = jnp.dot(h_s[...], wbuf[s3], preferred_element_type=F32)
            col = pl.ds(pl.multiple_of(i * TILE, TILE), TILE)
            u_s[:, col] = (a * jax.nn.sigmoid(a) * b).astype(BF16)
            start(t + NBUF)
            start(t + 1 + NBUF)

        @pl.loop(0, ny)
        def _(i):
            t = b_2 + kk * i
            acc = None
            for k in range(kk):
                slot = ready(t + k)
                r = jnp.dot(u_s[:, k * nk:(k + 1) * nk], wbuf[slot], preferred_element_type=F32)
                acc = r if acc is None else acc + r
            col = pl.ds(pl.multiple_of(i * TILE, TILE), TILE)
            y_ref[:, col] = (xm_s[:, col].astype(F32) + acc).astype(BF16)
            for k in range(kk):
                start(t + k + NBUF)

    if qkv:
        _norm_to(h_s, (y_ref if mlp else x_ref)[...], g1_ref[...])
        width = qkv_ref.shape[3]
        per = TILE // width

        @pl.loop(0, nq)
        def _(i):
            t = b_q + 3 * i
            for m in range(3):
                slot = ready(t + m)
                r = jnp.dot(h_s[...], wbuf[slot], preferred_element_type=F32)
                for a in range(TILE // HEAD):
                    z = r[:, a * HEAD:(a + 1) * HEAD]
                    if m < 2:
                        z = z * cos_ref[...] + pltpu.roll(z, HEAD // 2, 1) * sin_ref[...]
                    lane = (a * HEAD) % width
                    qkv_ref[i * per + (a * HEAD) // width, m, :, lane:lane + HEAD] = z.astype(BF16)
            for m in range(3):
                start(t + m + NBUF)


def _dense(layer, x, o, tabs, w, ncp, mlp, qkv):
    g1, g2, wq, wk, wv, wo, w1, w3, w2 = w
    rows, d = x.shape
    ff = w1.shape[2]
    width = wq.shape[2] // ncp
    anyspace = pl.BlockSpec(memory_space=pl.ANY)
    vmem = pl.BlockSpec(memory_space=pltpu.VMEM)
    ins, specs = [x], [vmem]
    outs, ospecs = [], []
    scratch = [pltpu.VMEM((rows, d), BF16), pltpu.VMEM((NBUF, d, TILE), BF16), pltpu.SemaphoreType.DMA((NBUF,))]
    flops = 0
    if mlp:
        ins += [o, g2[layer:layer + 1], wo, w1, w3, w2]
        specs += [vmem, vmem] + [anyspace] * 4
        outs.append(jax.ShapeDtypeStruct((rows, d), BF16))
        ospecs.append(vmem)
        scratch += [pltpu.VMEM((rows, d), BF16), pltpu.VMEM((rows, ff), BF16)]
        flops += 2 * rows * d * (d + 3 * ff)
    if qkv:
        ins += [g1[layer + 1:layer + 2], tabs[0], tabs[1], wq, wk, wv]
        specs += [vmem] * 3 + [anyspace] * 3
        outs.append(jax.ShapeDtypeStruct((ncp, 3, rows, width), BF16))
        ospecs.append(vmem)
        flops += 2 * rows * d * 3 * wq.shape[2]
    return pl.pallas_call(
        functools.partial(_dense_kernel, layer, mlp, qkv),
        out_shape=outs,
        in_specs=specs,
        out_specs=ospecs,
        scratch_shapes=scratch,
        compiler_params=pltpu.CompilerParams(vmem_limit_bytes=VMEM_LIMIT),
        cost_estimate=pl.CostEstimate(flops=flops, bytes_accessed=flops // rows, transcendentals=0),
        name=f"dense_{layer + 1}_{int(mlp)}{int(qkv)}",
    )(*ins)


def _attn_kernel(late, first, *refs):
    refs = list(refs)
    qkv_ref = refs.pop(0)
    pre_ref = refs.pop(0) if late else None
    if not first:
        refs = refs[2:]
    o_ref, kc_ref, vc_ref, acc_s, m_s, il_s = refs
    p = pl.program_id(0)
    npair = qkv_ref.shape[0] // 2
    seg, width = qkv_ref.shape[2], qkv_ref.shape[3]
    nh = width // HEAD
    bq = 2 * seg
    scale = HEAD ** -0.5 * math.log2(math.e)

    for which, out in ((1, kc_ref), (2, vc_ref)):
        for i in range(2):
            src = qkv_ref[2 * p + (1 - i if late else i), which]
            for h in range(nh):
                il_s[pl.ds(i * seg * nh + h, seg, stride=nh), :] = src[:, h * HEAD:(h + 1) * HEAD].astype(F32)
        out[0] = il_s[...].astype(BF16)

    ones = jnp.ones((bq, HEAD), BF16)

    def block(ref, j, which, h):
        return ref[pl.ds(2 * j, 2), which, :, h * HEAD:(h + 1) * HEAD].reshape(bq, HEAD)

    def wide(a, n):
        return jnp.concatenate([a] * n, axis=1)

    def scores(ref, j, h):
        return lax.dot_general(block(qkv_ref, p, 0, h), block(ref, j, 1, h), (((1,), (1,)), ((), ())),
                               preferred_element_type=F32)

    r = lax.broadcasted_iota(jnp.int32, (bq, bq), 0)
    c = lax.broadcasted_iota(jnp.int32, (bq, bq), 1)
    if late:
        r = jnp.where(r < seg, r + seg, r - seg)
        c = jnp.where(c < seg, c + seg, c - seg)
    mask = c <= r
    for h in range(nh):
        s = jnp.where(mask, scores(qkv_ref, p, h), -jnp.inf)
        m = jnp.broadcast_to(jnp.max(s, axis=1, keepdims=True), (bq, HEAD))
        pr = jnp.exp2((s - wide(m, bq // HEAD)) * scale).astype(BF16)
        v = jnp.concatenate([block(qkv_ref, p, 2, h), ones], axis=1)
        acc_s[h] = jnp.dot(pr, v, preferred_element_type=F32)
        m_s[h] = m

    def full(ref, j):
        for h in range(nh):
            s = scores(ref, j, h)
            old = m_s[h]
            m = jnp.maximum(old, jnp.broadcast_to(jnp.max(s, axis=1, keepdims=True), (bq, HEAD)))
            pr = jnp.exp2((s - wide(m, bq // HEAD)) * scale).astype(BF16)
            v = jnp.concatenate([block(ref, j, 2, h), ones], axis=1)
            alpha = jnp.exp2((old - m) * scale)
            acc_s[h] = acc_s[h] * wide(alpha, 2) + jnp.dot(pr, v, preferred_element_type=F32)
            m_s[h] = m

    if late:
        @pl.loop(0, npair)
        def _(j):
            full(pre_ref, j)

        @pl.loop(p + 1, npair)
        def _(j):
            full(qkv_ref, j)
    else:
        @pl.loop(0, p)
        def _(j):
            full(qkv_ref, j)

    for h in range(nh):
        o = (acc_s[h, :, :HEAD] / acc_s[h, :, HEAD:]).astype(BF16)
        o_ref[:, :, h * HEAD:(h + 1) * HEAD] = o.reshape(2, seg, HEAD)


def _attention(layer, layers, late, qkv, pre, caches):
    ncp, _, seg, width = qkv.shape
    nh = width // HEAD
    npair = ncp // 2
    rows = 2 * seg * nh
    whole = pl.BlockSpec((ncp, 3, seg, width), lambda p: (0, 0, 0, 0))
    ins, specs = [qkv], [whole]
    if late:
        ins.append(pre)
        specs.append(whole)
    alias = {}
    if caches is not None:
        alias = {len(ins): 1, len(ins) + 1: 2}
        ins += list(caches)
        specs += [pl.BlockSpec(memory_space=pl.ANY)] * 2
    where = (lambda p: (layer, 2 * npair - 1 - p, 0)) if late else (lambda p: (layer, p, 0))
    cache = jax.ShapeDtypeStruct((layers, 2 * ncp * seg * nh, HEAD), BF16)
    pairs = (ncp * seg) ** 2 // 2 * (3 if late else 1) * nh
    o, kc, vc = pl.pallas_call(
        functools.partial(_attn_kernel, late, caches is None),
        grid=(npair,),
        out_shape=[jax.ShapeDtypeStruct((ncp, seg, width), BF16), cache, cache],
        in_specs=specs,
        out_specs=[pl.BlockSpec((2, seg, width), lambda p: (p, 0, 0)),
                   pl.BlockSpec((1, rows, HEAD), where), pl.BlockSpec((1, rows, HEAD), where)],
        scratch_shapes=[pltpu.VMEM((nh, 2 * seg, 2 * HEAD), F32), pltpu.VMEM((nh, 2 * seg, HEAD), F32),
                        pltpu.VMEM((rows, HEAD), F32)],
        input_output_aliases=alias,
        compiler_params=pltpu.CompilerParams(vmem_limit_bytes=VMEM_LIMIT, dimension_semantics=("arbitrary",)),
        cost_estimate=pl.CostEstimate(flops=pairs * HEAD * 8, bytes_accessed=8 * ncp * seg * width * 2,
                                      transcendentals=pairs),
        name=f"attn_{layer}_{int(late)}",
    )(*ins)
    return o, (kc, vc)


def solution(mesh):
    ncp = mesh.shape['cp']
    act = P(('req', 'cp'), None)
    cache = P(None, 'req', 'cp', None)

    def swap(a):
        return lax.all_to_all(a, 'cp', 0, 0, tiled=True)

    def body(x, pos, g1, g2, wq, wk, wv, wo, w1, w3, w2):
        w = (g1, g2, wq, wk, wv, wo, w1, w3, w2)
        layers = wq.shape[0]
        seg = x.shape[0] // 2
        cos, sin = _tables(pos)
        tabs = [(cos[:seg], sin[:seg]), (cos[seg:], sin[seg:])]
        xs = [x[:seg], x[seg:]]
        qkv = [_dense(-1, xs[i], None, tabs[i], w, ncp, False, True)[0] for i in range(2)]
        caches = None
        for l in range(layers):
            more = l + 1 < layers
            ra = swap(qkv[0])
            qb, ra = lax.optimization_barrier((qkv[1], ra))
            rb = swap(qb)
            oa, caches = _attention(l, layers, False, ra, None, caches)
            res = _dense(l, xs[0], swap(oa), tabs[0], w, ncp, True, more)
            ob, caches = _attention(l, layers, True, rb, ra, caches)
            res_b = _dense(l, xs[1], swap(ob), tabs[1], w, ncp, True, more)
            xs = [res[0], res_b[0]]
            if more:
                qkv = [res[1], res_b[1]]
        kc, vc = (a.reshape(layers, -1, wq.shape[2] // ncp // HEAD, HEAD) for a in caches)
        return jnp.concatenate(xs, axis=0), kc, vc

    return jax.shard_map(body, mesh=mesh, in_specs=(act, P(('req', 'cp'))) + (P(),) * 9,
                         out_specs=(act, cache, cache), check_vma=False)
```

```python
import functools
import math

import jax
import jax.numpy as jnp
from jax import lax
from jax.experimental import pallas as pl
from jax.experimental.pallas import tpu as pltpu
from jax.sharding import PartitionSpec as P

HEAD = 128
TILE = 512
NBUF = 8
F32 = jnp.float32
BF16 = jnp.bfloat16
VMEM_LIMIT = 60 * 1024 * 1024


def _tables(pos):
    half = HEAD // 2
    inv = 1.0 / (10000.0 ** (jnp.arange(half, dtype=F32) * (2.0 / HEAD)))
    ang = pos.astype(F32)[:, None] * inv
    c, s = jnp.cos(ang), jnp.sin(ang)
    return jnp.concatenate([c, c], axis=1), jnp.concatenate([-s, s], axis=1)


def _norm_to(dst, x, g):
    x32 = x.astype(F32)
    r = lax.rsqrt(jnp.mean(x32 * x32, axis=-1, keepdims=True) + 1e-5)
    dst[...] = (x32 * r * g.astype(F32)).astype(BF16)


def _dense_kernel(layer, mlp, qkv, joined, *refs):
    refs = list(refs)
    x_ref = refs.pop(0)
    if mlp:
        o_ref, g2_ref, wo, w1, w3, w2 = refs[:6]
        refs = refs[6:]
    if qkv:
        g1_ref, cos_ref, sin_ref, wq, wk, wv = refs[:6]
        refs = refs[6:]
    if joined:
        refs.pop(0)
    if mlp:
        y_ref = refs.pop(0)
    if qkv:
        qkv_ref = refs.pop(0)
    h_s, wbuf, sems = refs[:3]
    if mlp:
        xm_s, u_s = refs[3:5]
    rows, d = x_ref.shape
    nk = wbuf.shape[1]

    segs = []
    base = 0
    if mlp:
        no, nf = wo.shape[2] // TILE, w1.shape[2] // TILE
        kk = w2.shape[1] // nk
        ny = w2.shape[2] // TILE
        b_o, b_1, b_2 = 0, no, no + 2 * nf
        segs.append((b_o, no, lambda i: [(None, wo.at[layer, :, pl.ds(i * TILE, TILE)])]))
        segs.append((b_1, 2 * nf, lambda i: [(0, w1.at[layer, :, pl.ds((i // 2) * TILE, TILE)]),
                                             (1, w3.at[layer, :, pl.ds((i // 2) * TILE, TILE)])]))
        segs.append((b_2, ny * kk, lambda i: [(None, w2.at[layer, pl.ds((i % kk) * nk, nk),
                                                          pl.ds((i // kk) * TILE, TILE)])]))
        base = b_2 + ny * kk
    if qkv:
        lq = layer + 1
        nq = wq.shape[2] // TILE
        b_q = base
        segs.append((b_q, 3 * nq, lambda i: [(0, wq.at[lq, :, pl.ds((i // 3) * TILE, TILE)]),
                                             (1, wk.at[lq, :, pl.ds((i // 3) * TILE, TILE)]),
                                             (2, wv.at[lq, :, pl.ds((i // 3) * TILE, TILE)])]))
        base = b_q + 3 * nq
    total = base

    def start(t):
        slot = lax.rem(t, NBUF) if not isinstance(t, int) else t % NBUF
        for b, n, srcs in segs:
            if isinstance(t, int):
                if b <= t < b + n:
                    lst = srcs(t - b)
                    src = lst[(t - b) % len(lst)][1]
                    pltpu.make_async_copy(src, wbuf.at[slot], sems.at[slot]).start()
                continue
            i = t - b
            lst = srcs(i)
            for which, src in lst:
                cond = (t >= b) & (t < b + n)
                if which is not None:
                    cond = cond & (lax.rem(i, len(lst)) == which)

                @pl.when(cond)
                def _(src=src):
                    pltpu.make_async_copy(src, wbuf.at[slot], sems.at[slot]).start()

    any_src = segs[0][2](0)[0][1]

    def ready(t):
        slot = lax.rem(t, NBUF)
        pltpu.make_async_copy(any_src, wbuf.at[slot], sems.at[slot]).wait()
        return slot

    for t in range(min(NBUF, total)):
        start(t)

    if mlp:
        for j in range(o_ref.shape[0]):
            w = o_ref.shape[2]
            h_s[:, j * w:(j + 1) * w] = o_ref[j]

        @pl.loop(0, no)
        def _(i):
            t = b_o + i
            slot = ready(t)
            col = pl.ds(pl.multiple_of(i * TILE, TILE), TILE)
            r = jnp.dot(h_s[...], wbuf[slot], preferred_element_type=F32)
            xm_s[:, col] = (x_ref[:, col].astype(F32) + r).astype(BF16)
            start(t + NBUF)

        _norm_to(h_s, xm_s[...], g2_ref[...])

        @pl.loop(0, nf)
        def _(i):
            t = b_1 + 2 * i
            s1 = ready(t)
            s3 = ready(t + 1)
            a = jnp.dot(h_s[...], wbuf[s1], preferred_element_type=F32)
            b = jnp.dot(h_s[...], wbuf[s3], preferred_element_type=F32)
            col = pl.ds(pl.multiple_of(i * TILE, TILE), TILE)
            u_s[:, col] = (a * jax.nn.sigmoid(a) * b).astype(BF16)
            start(t + NBUF)
            start(t + 1 + NBUF)

        @pl.loop(0, ny)
        def _(i):
            t = b_2 + kk * i
            acc = None
            slots = [ready(t + k) for k in range(kk)]
            for k in range(kk):
                r = jnp.dot(u_s[:, k * nk:(k + 1) * nk], wbuf[slots[k]], preferred_element_type=F32)
                acc = r if acc is None else acc + r
            col = pl.ds(pl.multiple_of(i * TILE, TILE), TILE)
            y_ref[:, col] = (xm_s[:, col].astype(F32) + acc).astype(BF16)
            for k in range(kk):
                start(t + k + NBUF)

    if qkv:
        _norm_to(h_s, (y_ref if mlp else x_ref)[...], g1_ref[...])
        width = qkv_ref.shape[3]
        per = TILE // width

        @pl.loop(0, nq)
        def _(i):
            t = b_q + 3 * i
            slots = [ready(t + m) for m in range(3)]
            for m in range(3):
                r = jnp.dot(h_s[...], wbuf[slots[m]], preferred_element_type=F32)
                for a in range(TILE // HEAD):
                    z = r[:, a * HEAD:(a + 1) * HEAD]
                    if m < 2:
                        z = z * cos_ref[...] + pltpu.roll(z, HEAD // 2, 1) * sin_ref[...]
                    lane = (a * HEAD) % width
                    qkv_ref[i * per + (a * HEAD) // width, m, :, lane:lane + HEAD] = z.astype(BF16)
            for m in range(3):
                start(t + m + NBUF)


def _dense(layer, half, x, o, tabs, w, ncp, mlp, qkv, y=None):
    g1, g2, wq, wk, wv, wo, w1, w3, w2 = w
    rows = tabs[0].shape[0] // 2
    d = x.shape[1]
    ff = w1.shape[2]
    width = wq.shape[2] // ncp
    anyspace = pl.BlockSpec(memory_space=pl.ANY)
    vmem = pl.BlockSpec(memory_space=pltpu.VMEM)

    def part(a):
        return pl.BlockSpec((rows, a.shape[1]), lambda i: (half if a.shape[0] > rows else 0, 0))

    def whole(a):
        return pl.BlockSpec(a.shape, lambda i: (0,) * len(a.shape))

    ins, specs = [x], [part(x)]
    outs, ospecs = [], []
    scratch = [pltpu.VMEM((rows, d), BF16), pltpu.VMEM((NBUF, d, TILE), BF16), pltpu.SemaphoreType.DMA((NBUF,))]
    flops = 0
    alias = {}
    if mlp:
        g = g2[layer:layer + 1]
        ins += [o, g, wo, w1, w3, w2]
        specs += [whole(o), whole(g)] + [anyspace] * 4
        outs.append(jax.ShapeDtypeStruct((rows if qkv else 2 * rows, d), BF16))
        ospecs.append(part(outs[-1]))
        scratch += [pltpu.VMEM((rows, d), BF16), pltpu.VMEM((rows, ff), BF16)]
        flops += 2 * rows * d * (d + 3 * ff)
    if qkv:
        g = g1[layer + 1:layer + 2]
        ins += [g, tabs[0], tabs[1], wq, wk, wv]
        specs += [whole(g), part(tabs[0]), part(tabs[1])] + [anyspace] * 3
        outs.append(jax.ShapeDtypeStruct((ncp, 3, rows, width), BF16))
        ospecs.append(whole(outs[-1]))
        flops += 2 * rows * d * 3 * wq.shape[2]
    if y is not None:
        alias = {len(ins): 0}
        ins.append(y)
        specs.append(anyspace)
    return pl.pallas_call(
        functools.partial(_dense_kernel, layer, mlp, qkv, y is not None),
        grid=(1,),
        out_shape=outs,
        in_specs=specs,
        out_specs=ospecs,
        scratch_shapes=scratch,
        input_output_aliases=alias,
        compiler_params=pltpu.CompilerParams(vmem_limit_bytes=VMEM_LIMIT, dimension_semantics=("arbitrary",)),
        cost_estimate=pl.CostEstimate(flops=flops, bytes_accessed=flops // rows, transcendentals=0),
        name=f"dense_{layer + 1}_{half}",
    )(*ins)


def _cache_kernel(first, ra_ref, rb_ref, *refs):
    kc_ref, vc_ref, il_s = refs if first else refs[2:]
    n = pl.program_id(0)
    half = pl.num_programs(0) // 2
    seg, width = ra_ref.shape[2], ra_ref.shape[3]
    nh = width // HEAD

    def write(ref, order):
        for which, out in ((1, kc_ref), (2, vc_ref)):
            for i in range(2):
                src = ref[order[i], which]
                for h in range(nh):
                    il_s[which - 1, pl.ds(i * seg * nh + h, seg, stride=nh), :] = (
                        src[:, h * HEAD:(h + 1) * HEAD].astype(F32))
            out[0] = il_s[which - 1].astype(BF16)

    @pl.when(n < half)
    def _():
        write(ra_ref, (0, 1))

    @pl.when(n >= half)
    def _():
        write(rb_ref, (1, 0))


def _cache(layer, layers, ra, rb, caches):
    ncp, _, seg, width = ra.shape
    nh = width // HEAD
    npair = ncp // 2
    rows = 2 * seg * nh
    ins = [ra, rb]
    specs = [pl.BlockSpec((2, 3, seg, width), lambda n: (jnp.minimum(n, npair - 1), 0, 0, 0)),
             pl.BlockSpec((2, 3, seg, width), lambda n: (jnp.minimum(2 * npair - 1 - n, npair - 1), 0, 0, 0))]
    alias = {}
    if caches is not None:
        alias = {2: 0, 3: 1}
        ins += list(caches)
        specs += [pl.BlockSpec(memory_space=pl.ANY)] * 2
    cache = jax.ShapeDtypeStruct((layers, 2 * ncp * seg * nh, HEAD), BF16)
    spec = pl.BlockSpec((1, rows, HEAD), lambda n: (layer, n, 0))
    return pl.pallas_call(
        functools.partial(_cache_kernel, caches is None),
        grid=(2 * npair,),
        out_shape=[cache, cache],
        in_specs=specs,
        out_specs=[spec, spec],
        scratch_shapes=[pltpu.VMEM((2, rows, HEAD), F32)],
        input_output_aliases=alias,
        compiler_params=pltpu.CompilerParams(dimension_semantics=("arbitrary",)),
        cost_estimate=pl.CostEstimate(flops=4 * 10 ** 9, bytes_accessed=10 * ncp * seg * width * 2,
                                      transcendentals=0),
        name=f"cache_{layer}",
    )(*ins)


def _attn_kernel(late, *refs):
    refs = list(refs)
    qkv_ref = refs.pop(0)
    pre_ref = refs.pop(0) if late else None
    out_ref, o_s, acc_s, m_s, send_sem, recv_sem = refs
    me = lax.axis_index('cp')
    step = pl.program_id(0)
    ncp = qkv_ref.shape[0]
    npair = ncp // 2
    seg, width = qkv_ref.shape[2], qkv_ref.shape[3]
    nh = width // HEAD
    bq = 2 * seg
    scale = HEAD ** -0.5 * math.log2(math.e)
    p = lax.rem(me // 2 + 1 + step, npair)
    barrier = pltpu.get_barrier_semaphore()

    @pl.when(step == 0)
    def _():
        for i in range(1, ncp):
            pl.semaphore_signal(barrier, inc=1, device_id={'cp': lax.rem(me + i, ncp)},
                                device_id_type=pl.DeviceIdType.MESH)

    ones = jnp.ones((bq, HEAD), BF16)

    def block(ref, j, which, h):
        return ref[pl.ds(2 * j, 2), which, :, h * HEAD:(h + 1) * HEAD].reshape(bq, HEAD)

    def wide(a, n):
        return jnp.concatenate([a] * n, axis=1)

    def scores(ref, j, h):
        return lax.dot_general(block(qkv_ref, p, 0, h), block(ref, j, 1, h), (((1,), (1,)), ((), ())),
                               preferred_element_type=F32)

    r = lax.broadcasted_iota(jnp.int32, (bq, bq), 0)
    c = lax.broadcasted_iota(jnp.int32, (bq, bq), 1)
    if late:
        r = jnp.where(r < seg, r + seg, r - seg)
        c = jnp.where(c < seg, c + seg, c - seg)
    mask = c <= r
    for h in range(nh):
        s = jnp.where(mask, scores(qkv_ref, p, h), -jnp.inf)
        m = jnp.broadcast_to(jnp.max(s, axis=1, keepdims=True), (bq, HEAD))
        pr = jnp.exp2((s - wide(m, bq // HEAD)) * scale).astype(BF16)
        v = jnp.concatenate([block(qkv_ref, p, 2, h), ones], axis=1)
        acc_s[h] = jnp.dot(pr, v, preferred_element_type=F32)
        m_s[h] = m

    def full(ref, j):
        ss = [scores(ref, j, h) for h in range(nh)]
        for h in range(nh):
            s = ss[h]
            old = m_s[h]
            m = jnp.maximum(old, jnp.broadcast_to(jnp.max(s, axis=1, keepdims=True), (bq, HEAD)))
            pr = jnp.exp2((s - wide(m, bq // HEAD)) * scale).astype(BF16)
            v = jnp.concatenate([block(ref, j, 2, h), ones], axis=1)
            alpha = jnp.exp2((old - m) * scale)
            acc_s[h] = acc_s[h] * wide(alpha, 2) + jnp.dot(pr, v, preferred_element_type=F32)
            m_s[h] = m

    if late:
        @pl.loop(0, npair)
        def _(j):
            full(pre_ref, j)

        @pl.loop(p + 1, npair)
        def _(j):
            full(qkv_ref, j)
    else:
        @pl.loop(0, p)
        def _(j):
            full(qkv_ref, j)

    for h in range(nh):
        o = (acc_s[h, :, :HEAD] / acc_s[h, :, HEAD:]).astype(BF16)
        o_s[pl.ds(2 * p, 2), :, h * HEAD:(h + 1) * HEAD] = o.reshape(2, seg, HEAD)

    @pl.when(step == 0)
    def _():
        pl.semaphore_wait(barrier, ncp - 1)

    def remote(j, slot):
        return pltpu.make_async_remote_copy(
            src_ref=o_s.at[j], dst_ref=out_ref.at[slot], send_sem=send_sem.at[j], recv_sem=recv_sem.at[slot],
            device_id={'cp': j}, device_id_type=pl.DeviceIdType.MESH)

    def local():
        return pltpu.make_async_copy(o_s.at[me], out_ref.at[me], recv_sem.at[me])

    for a in range(2):
        j = 2 * p + a

        @pl.when(j != me)
        def _():
            remote(j, me).start()

        @pl.when(j == me)
        def _():
            local().start()

    @pl.when(step == npair - 1)
    def _():
        local().wait()
        for i in range(1, ncp):
            j = lax.rem(me + i, ncp)
            remote(j, me).wait_send()
            remote(j, j).wait_recv()


def _attention(layer, late, qkv, pre):
    ncp, _, seg, width = qkv.shape
    nh = width // HEAD
    npair = ncp // 2
    whole = pl.BlockSpec((ncp, 3, seg, width), lambda p: (0, 0, 0, 0))
    pairs = (ncp * seg) ** 2 // 2 * (3 if late else 1) * nh
    return pl.pallas_call(
        functools.partial(_attn_kernel, late),
        grid=(npair,),
        out_shape=jax.ShapeDtypeStruct((ncp, seg, width), BF16),
        in_specs=[whole] * (2 if late else 1),
        out_specs=pl.BlockSpec(memory_space=pl.ANY),
        scratch_shapes=[pltpu.VMEM((ncp, seg, width), BF16),
                        pltpu.VMEM((nh, 2 * seg, 2 * HEAD), F32), pltpu.VMEM((nh, 2 * seg, HEAD), F32),
                        pltpu.SemaphoreType.DMA((ncp,)), pltpu.SemaphoreType.DMA((ncp,))],
        compiler_params=pltpu.CompilerParams(vmem_limit_bytes=VMEM_LIMIT, dimension_semantics=("arbitrary",),
                                             collective_id=2 * layer + int(late), has_side_effects=True),
        cost_estimate=pl.CostEstimate(flops=pairs * HEAD * 8, bytes_accessed=8 * ncp * seg * width * 2,
                                      transcendentals=pairs),
        name=f"attn_{layer}_{int(late)}",
    )(*((qkv, pre) if late else (qkv,)))


def solution(mesh):
    ncp = mesh.shape['cp']
    act = P(('req', 'cp'), None)
    cache = P(None, 'req', 'cp', None)

    def swap(a):
        return lax.all_to_all(a, 'cp', 0, 0, tiled=True)

    def after(a, *deps):
        return lax.optimization_barrier((a,) + deps)[0]

    def body(x, pos, g1, g2, wq, wk, wv, wo, w1, w3, w2):
        w = (g1, g2, wq, wk, wv, wo, w1, w3, w2)
        layers = wq.shape[0]
        tabs = _tables(pos)
        xs = [x, x]
        qkv = [_dense(-1, i, x, None, tabs, w, ncp, False, True)[0] for i in range(2)]
        caches = None
        for l in range(layers):
            more = l + 1 < layers
            ra = swap(qkv[0])
            rb = swap(after(qkv[1], ra))
            oa = _attention(l, False, ra, None)
            res = _dense(l, 0, xs[0], oa, tabs, w, ncp, True, more)
            ob = _attention(l, True, after(rb, res[0]), ra)
            caches = _cache(l, layers, ra, rb, caches)
            res_b = _dense(l, 1, xs[1], ob, tabs, w, ncp, True, more, None if more else res[0])
            xs = [res[0], res_b[0]]
            if more:
                qkv = [res[1], res_b[1]]
        kc, vc = (a.reshape(layers, -1, wq.shape[2] // ncp // HEAD, HEAD) for a in caches)
        return xs[1], kc, vc

    return jax.shard_map(body, mesh=mesh, in_specs=(act, P(('req', 'cp'))) + (P(),) * 9,
                         out_specs=(act, cache, cache), check_vma=False)
```

```python
import functools
import math

import jax
import jax.numpy as jnp
from jax import lax
from jax.experimental import pallas as pl
from jax.experimental.pallas import tpu as pltpu
from jax.sharding import PartitionSpec as P

HEAD = 128
TILE = 512
NBUF = 8
RING = 14
F32 = jnp.float32
BF16 = jnp.bfloat16
VMEM_LIMIT = 60 * 1024 * 1024


def _tables(pos):
    half = HEAD // 2
    inv = 1.0 / (10000.0 ** (jnp.arange(half, dtype=F32) * (2.0 / HEAD)))
    ang = pos.astype(F32)[:, None] * inv
    c, s = jnp.cos(ang), jnp.sin(ang)
    return jnp.concatenate([c, c], axis=1), jnp.concatenate([-s, s], axis=1)


def _norm_to(dst, x, g):
    x32 = x.astype(F32)
    r = lax.rsqrt(jnp.mean(x32 * x32, axis=-1, keepdims=True) + 1e-5)
    dst[...] = (x32 * r * g.astype(F32)).astype(BF16)


def _dense_kernel(layer, mlp, qkv, joined, *refs):
    refs = list(refs)
    x_ref = refs.pop(0)
    if mlp:
        o_ref, g2_ref, wo, w1, w3, w2 = refs[:6]
        refs = refs[6:]
    if qkv:
        g1_ref, cos_ref, sin_ref, wq, wk, wv = refs[:6]
        refs = refs[6:]
    if joined:
        refs.pop(0)
    if mlp:
        y_ref = refs.pop(0)
    if qkv:
        qkv_ref = refs.pop(0)
    h_s, wbuf, sems = refs[:3]
    if mlp:
        xm_s, u_s = refs[3:5]
    rows, d = x_ref.shape
    nk = wbuf.shape[1]

    segs = []
    base = 0
    if mlp:
        no, nf = wo.shape[2] // TILE, w1.shape[2] // TILE
        kk = w2.shape[1] // nk
        ny = w2.shape[2] // TILE
        b_o, b_1, b_2 = 0, no, no + 2 * nf
        segs.append((b_o, no, lambda i: [(None, wo.at[layer, :, pl.ds(i * TILE, TILE)])]))
        segs.append((b_1, 2 * nf, lambda i: [(0, w1.at[layer, :, pl.ds((i // 2) * TILE, TILE)]),
                                             (1, w3.at[layer, :, pl.ds((i // 2) * TILE, TILE)])]))
        segs.append((b_2, ny * kk, lambda i: [(None, w2.at[layer, pl.ds((i % kk) * nk, nk),
                                                          pl.ds((i // kk) * TILE, TILE)])]))
        base = b_2 + ny * kk
    if qkv:
        lq = layer + 1
        nq = wq.shape[2] // TILE
        b_q = base
        segs.append((b_q, 3 * nq, lambda i: [(0, wq.at[lq, :, pl.ds((i // 3) * TILE, TILE)]),
                                             (1, wk.at[lq, :, pl.ds((i // 3) * TILE, TILE)]),
                                             (2, wv.at[lq, :, pl.ds((i // 3) * TILE, TILE)])]))
        base = b_q + 3 * nq
    total = base

    def start(t):
        slot = lax.rem(t, NBUF) if not isinstance(t, int) else t % NBUF
        for b, n, srcs in segs:
            if isinstance(t, int):
                if b <= t < b + n:
                    lst = srcs(t - b)
                    src = lst[(t - b) % len(lst)][1]
                    pltpu.make_async_copy(src, wbuf.at[slot], sems.at[slot]).start()
                continue
            i = t - b
            lst = srcs(i)
            for which, src in lst:
                cond = (t >= b) & (t < b + n)
                if which is not None:
                    cond = cond & (lax.rem(i, len(lst)) == which)

                @pl.when(cond)
                def _(src=src):
                    pltpu.make_async_copy(src, wbuf.at[slot], sems.at[slot]).start()

    any_src = segs[0][2](0)[0][1]

    def ready(t):
        slot = lax.rem(t, NBUF)
        pltpu.make_async_copy(any_src, wbuf.at[slot], sems.at[slot]).wait()
        return slot

    for t in range(min(NBUF, total)):
        start(t)

    if mlp:
        for j in range(o_ref.shape[0]):
            w = o_ref.shape[2]
            h_s[:, j * w:(j + 1) * w] = o_ref[j]

        @pl.loop(0, no)
        def _(i):
            t = b_o + i
            slot = ready(t)
            col = pl.ds(pl.multiple_of(i * TILE, TILE), TILE)
            r = jnp.dot(h_s[...], wbuf[slot], preferred_element_type=F32)
            xm_s[:, col] = (x_ref[:, col].astype(F32) + r).astype(BF16)
            start(t + NBUF)

        _norm_to(h_s, xm_s[...], g2_ref[...])

        @pl.loop(0, nf)
        def _(i):
            t = b_1 + 2 * i
            s1 = ready(t)
            s3 = ready(t + 1)
            a = jnp.dot(h_s[...], wbuf[s1], preferred_element_type=F32)
            b = jnp.dot(h_s[...], wbuf[s3], preferred_element_type=F32)
            col = pl.ds(pl.multiple_of(i * TILE, TILE), TILE)
            u_s[:, col] = (a * jax.nn.sigmoid(a) * b).astype(BF16)
            start(t + NBUF)
            start(t + 1 + NBUF)

        @pl.loop(0, ny)
        def _(i):
            t = b_2 + kk * i
            acc = None
            slots = [ready(t + k) for k in range(kk)]
            for k in range(kk):
                r = jnp.dot(u_s[:, k * nk:(k + 1) * nk], wbuf[slots[k]], preferred_element_type=F32)
                acc = r if acc is None else acc + r
            col = pl.ds(pl.multiple_of(i * TILE, TILE), TILE)
            y_ref[:, col] = (xm_s[:, col].astype(F32) + acc).astype(BF16)
            for k in range(kk):
                start(t + k + NBUF)

    if qkv:
        _norm_to(h_s, (y_ref if mlp else x_ref)[...], g1_ref[...])
        width = qkv_ref.shape[3]
        per = TILE // width

        @pl.loop(0, nq)
        def _(i):
            t = b_q + 3 * i
            slots = [ready(t + m) for m in range(3)]
            for m in range(3):
                r = jnp.dot(h_s[...], wbuf[slots[m]], preferred_element_type=F32)
                for a in range(TILE // HEAD):
                    z = r[:, a * HEAD:(a + 1) * HEAD]
                    if m < 2:
                        z = z * cos_ref[...] + pltpu.roll(z, HEAD // 2, 1) * sin_ref[...]
                    lane = (a * HEAD) % width
                    qkv_ref[i * per + (a * HEAD) // width, m, :, lane:lane + HEAD] = z.astype(BF16)
            for m in range(3):
                start(t + m + NBUF)


def _dense(layer, half, x, o, tabs, w, ncp, mlp, qkv, y=None):
    g1, g2, wq, wk, wv, wo, w1, w3, w2 = w
    rows = tabs[0].shape[0] // 2
    d = x.shape[1]
    ff = w1.shape[2]
    width = wq.shape[2] // ncp
    anyspace = pl.BlockSpec(memory_space=pl.ANY)
    vmem = pl.BlockSpec(memory_space=pltpu.VMEM)

    def part(a):
        return pl.BlockSpec((rows, a.shape[1]), lambda i: (half if a.shape[0] > rows else 0, 0))

    def whole(a):
        return pl.BlockSpec(a.shape, lambda i: (0,) * len(a.shape))

    ins, specs = [x], [part(x)]
    outs, ospecs = [], []
    scratch = [pltpu.VMEM((rows, d), BF16), pltpu.VMEM((NBUF, d, TILE), BF16), pltpu.SemaphoreType.DMA((NBUF,))]
    flops = 0
    alias = {}
    if mlp:
        g = g2[layer:layer + 1]
        ins += [o, g, wo, w1, w3, w2]
        specs += [whole(o), whole(g)] + [anyspace] * 4
        outs.append(jax.ShapeDtypeStruct((rows if qkv else 2 * rows, d), BF16))
        ospecs.append(part(outs[-1]))
        scratch += [pltpu.VMEM((rows, d), BF16), pltpu.VMEM((rows, ff), BF16)]
        flops += 2 * rows * d * (d + 3 * ff)
    if qkv:
        g = g1[layer + 1:layer + 2]
        ins += [g, tabs[0], tabs[1], wq, wk, wv]
        specs += [whole(g), part(tabs[0]), part(tabs[1])] + [anyspace] * 3
        outs.append(jax.ShapeDtypeStruct((ncp, 3, rows, width), BF16))
        ospecs.append(whole(outs[-1]))
        flops += 2 * rows * d * 3 * wq.shape[2]
    if y is not None:
        alias = {len(ins): 0}
        ins.append(y)
        specs.append(anyspace)
    return pl.pallas_call(
        functools.partial(_dense_kernel, layer, mlp, qkv, y is not None),
        grid=(1,),
        out_shape=outs,
        in_specs=specs,
        out_specs=ospecs,
        scratch_shapes=scratch,
        input_output_aliases=alias,
        compiler_params=pltpu.CompilerParams(vmem_limit_bytes=VMEM_LIMIT, dimension_semantics=("arbitrary",)),
        cost_estimate=pl.CostEstimate(flops=flops, bytes_accessed=flops // rows, transcendentals=0),
        name=f"dense_{layer + 1}_{half}",
    )(*ins)


def _cache_kernel(first, ka_ref, va_ref, kb_ref, vb_ref, *refs):
    kc_ref, vc_ref, il_s = refs if first else refs[2:]
    n = pl.program_id(0)
    half = pl.num_programs(0) // 2
    seg, width = ka_ref.shape[2], ka_ref.shape[3]
    nh = width // HEAD

    def write(pair, order):
        for which, out in ((1, kc_ref), (2, vc_ref)):
            for i in range(2):
                src = pair[which - 1][order[i], 0]
                for h in range(nh):
                    il_s[which - 1, pl.ds(i * seg * nh + h, seg, stride=nh), :] = (
                        src[:, h * HEAD:(h + 1) * HEAD].astype(F32))
            out[0] = il_s[which - 1].astype(BF16)

    @pl.when(n < half)
    def _():
        write((ka_ref, va_ref), (0, 1))

    @pl.when(n >= half)
    def _():
        write((kb_ref, vb_ref), (1, 0))


def _cache(layer, layers, ra, rb, caches):
    ncp, _, seg, width = ra.shape
    nh = width // HEAD
    npair = ncp // 2
    rows = 2 * seg * nh
    ins = [ra, ra, rb, rb]
    block = (2, 1, seg, width)
    specs = [pl.BlockSpec(block, lambda n, m=m: (jnp.minimum(n, npair - 1), m, 0, 0)) for m in (1, 2)]
    specs += [pl.BlockSpec(block, lambda n, m=m: (jnp.minimum(2 * npair - 1 - n, npair - 1), m, 0, 0)) for m in (1, 2)]
    alias = {}
    if caches is not None:
        alias = {4: 0, 5: 1}
        ins += list(caches)
        specs += [pl.BlockSpec(memory_space=pl.ANY)] * 2
    cache = jax.ShapeDtypeStruct((layers, 2 * ncp * seg * nh, HEAD), BF16)
    spec = pl.BlockSpec((1, rows, HEAD), lambda n: (layer, n, 0))
    return pl.pallas_call(
        functools.partial(_cache_kernel, caches is None),
        grid=(2 * npair,),
        out_shape=[cache, cache],
        in_specs=specs,
        out_specs=[spec, spec],
        scratch_shapes=[pltpu.VMEM((2, rows, HEAD), F32)],
        input_output_aliases=alias,
        compiler_params=pltpu.CompilerParams(dimension_semantics=("arbitrary",)),
        cost_estimate=pl.CostEstimate(flops=4 * 10 ** 9, bytes_accessed=10 * ncp * seg * width * 2,
                                      transcendentals=0),
        name=f"cache_{layer}",
    )(*ins)


def _layer_kernel(layer, late, more, swap, joined, *refs):
    refs = list(refs)
    x_ref, qkv_ref = refs[:2]
    refs = refs[2:]
    pre_ref = refs.pop(0) if late else None
    g2_ref, wo, w1, w3, w2 = refs[:5]
    refs = refs[5:]
    if more:
        g1_ref, cos_ref, sin_ref, wq, wk, wv = refs[:6]
        refs = refs[6:]
    if swap:
        ex_in = refs.pop(0)
    if joined:
        refs.pop(0)
    y_ref = refs.pop(0)
    if more:
        nxt_ref = refs.pop(0)
    if swap:
        ex_out = refs.pop(0)
    h_s, wbuf, sems, xm_s, u_s, o_s, o_r, acc_s, m_s, send_sem, recv_sem, out_sem = refs[:12]
    if swap:
        xs_sem, xr_sem = refs[12:]
    nbuf = wbuf.shape[0]
    half = int(late)
    rows, d = h_s.shape
    nk = wbuf.shape[1]
    ncp, _, seg, width = qkv_ref.shape
    npair = ncp // 2
    nh = width // HEAD
    bq = 2 * seg
    scale = HEAD ** -0.5 * math.log2(math.e)
    me = lax.axis_index('cp')
    barrier = pltpu.get_barrier_semaphore()
    for i in range(1, ncp):
        pl.semaphore_signal(barrier, inc=1, device_id={'cp': lax.rem(me + i, ncp)},
                            device_id_type=pl.DeviceIdType.MESH)

    def col(i):
        return pl.ds(i * TILE, TILE)

    no, nf = wo.shape[2] // TILE, w1.shape[2] // TILE
    kk, ny = w2.shape[1] // nk, w2.shape[2] // TILE
    b_o, b_1, b_2 = 0, no, no + 2 * nf
    b_q = b_2 + ny * kk
    segs = [(b_o, no, lambda i: [wo.at[layer, :, col(i)]]),
            (b_1, 2 * nf, lambda i: [w1.at[layer, :, col(i // 2)], w3.at[layer, :, col(i // 2)]]),
            (b_2, ny * kk, lambda i: [w2.at[layer, pl.ds((i % kk) * nk, nk), col(i // kk)]])]
    if more:
        nq = wq.shape[2] // TILE
        segs.append((b_q, 3 * nq, lambda i: [w.at[layer + 1, :, col(i // 3)] for w in (wq, wk, wv)]))

    def start(t):
        slot = t % nbuf if isinstance(t, int) else lax.rem(t, nbuf)
        for first, n, srcs in segs:
            if isinstance(t, int):
                if first <= t < first + n:
                    lst = srcs(t - first)
                    pltpu.make_async_copy(lst[(t - first) % len(lst)], wbuf.at[slot], sems.at[slot]).start()
                continue
            i = t - first
            lst = srcs(i)
            for which, src in enumerate(lst):
                cond = (t >= first) & (t < first + n)
                if len(lst) > 1:
                    cond = cond & (lax.rem(i, len(lst)) == which)

                @pl.when(cond)
                def _(src=src):
                    pltpu.make_async_copy(src, wbuf.at[slot], sems.at[slot]).start()

    def ready(t):
        slot = lax.rem(t, nbuf)
        pltpu.make_async_copy(wo.at[layer, :, col(0)], wbuf.at[slot], sems.at[slot]).wait()
        return slot

    for t in range(nbuf):
        start(t)

    ones = jnp.ones((bq, HEAD), BF16)

    def block(ref, j, which, h):
        return ref[pl.ds(2 * j, 2), which, :, h * HEAD:(h + 1) * HEAD].reshape(bq, HEAD)

    def wide(a, n):
        return jnp.concatenate([a] * n, axis=1)

    def remote(j, slot):
        return pltpu.make_async_remote_copy(
            src_ref=o_s.at[j], dst_ref=o_r.at[slot], send_sem=send_sem.at[j], recv_sem=recv_sem.at[slot],
            device_id={'cp': j}, device_id_type=pl.DeviceIdType.MESH)

    def local():
        return pltpu.make_async_copy(o_s.at[me], o_r.at[me], recv_sem.at[me])

    @pl.loop(0, npair)
    def _(step):
        p = lax.rem(me // 2 + 1 + step, npair)

        def scores(ref, j, h):
            return lax.dot_general(block(qkv_ref, p, 0, h), block(ref, j, 1, h), (((1,), (1,)), ((), ())),
                                   preferred_element_type=F32)

        r = lax.broadcasted_iota(jnp.int32, (bq, bq), 0)
        c = lax.broadcasted_iota(jnp.int32, (bq, bq), 1)
        if late:
            r = jnp.where(r < seg, r + seg, r - seg)
            c = jnp.where(c < seg, c + seg, c - seg)
        mask = c <= r
        for h in range(nh):
            s = jnp.where(mask, scores(qkv_ref, p, h), -jnp.inf)
            m = jnp.broadcast_to(jnp.max(s, axis=1, keepdims=True), (bq, HEAD))
            pr = jnp.exp2((s - wide(m, bq // HEAD)) * scale).astype(BF16)
            v = jnp.concatenate([block(qkv_ref, p, 2, h), ones], axis=1)
            acc_s[h] = jnp.dot(pr, v, preferred_element_type=F32)
            m_s[h] = m

        def full(ref, j):
            ss = [scores(ref, j, h) for h in range(nh)]
            for h in range(nh):
                s = ss[h]
                old = m_s[h]
                m = jnp.maximum(old, jnp.broadcast_to(jnp.max(s, axis=1, keepdims=True), (bq, HEAD)))
                pr = jnp.exp2((s - wide(m, bq // HEAD)) * scale).astype(BF16)
                v = jnp.concatenate([block(ref, j, 2, h), ones], axis=1)
                alpha = jnp.exp2((old - m) * scale)
                acc_s[h] = acc_s[h] * wide(alpha, 2) + jnp.dot(pr, v, preferred_element_type=F32)
                m_s[h] = m

        if late:
            @pl.loop(0, npair)
            def _(j):
                full(pre_ref, j)

            @pl.loop(p + 1, npair)
            def _(j):
                full(qkv_ref, j)
        else:
            @pl.loop(0, p)
            def _(j):
                full(qkv_ref, j)

        for h in range(nh):
            o = (acc_s[h, :, :HEAD] / acc_s[h, :, HEAD:]).astype(BF16)
            o_s[pl.ds(2 * p, 2), :, h * HEAD:(h + 1) * HEAD] = o.reshape(2, seg, HEAD)

        @pl.when(step == 0)
        def _():
            pl.semaphore_wait(barrier, ncp - 1)

        for a in range(2):
            j = 2 * p + a

            @pl.when(j != me)
            def _():
                remote(j, me).start()

            @pl.when(j == me)
            def _():
                local().start()

    def cross(j, slot):
        return pltpu.make_async_remote_copy(
            src_ref=ex_in.at[j], dst_ref=ex_out.at[slot], send_sem=xs_sem.at[j], recv_sem=xr_sem.at[slot],
            device_id={'cp': j}, device_id_type=pl.DeviceIdType.MESH)

    def keep():
        return pltpu.make_async_copy(ex_in.at[me], ex_out.at[me], xr_sem.at[me])

    if swap:
        for i in range(1, ncp):
            cross(lax.rem(me + i, ncp), me).start()
        keep().start()

    local().wait()
    for i in range(1, ncp):
        j = lax.rem(me + i, ncp)
        remote(j, me).wait_send()
        remote(j, j).wait_recv()

    for j in range(ncp):
        h_s[:, j * width:(j + 1) * width] = o_r[j]
    x_at = half * rows if x_ref.shape[0] > rows else 0

    @pl.loop(0, no)
    def _(i):
        t = b_o + i
        slot = ready(t)
        cs = pl.ds(pl.multiple_of(i * TILE, TILE), TILE)
        r = jnp.dot(h_s[...], wbuf[slot], preferred_element_type=F32)
        xm_s[:, cs] = (x_ref[x_at:x_at + rows, cs].astype(F32) + r).astype(BF16)
        start(t + nbuf)

    _norm_to(h_s, xm_s[...], g2_ref[...])

    @pl.loop(0, nf)
    def _(i):
        t = b_1 + 2 * i
        s1 = ready(t)
        s3 = ready(t + 1)
        a = jnp.dot(h_s[...], wbuf[s1], preferred_element_type=F32)
        b = jnp.dot(h_s[...], wbuf[s3], preferred_element_type=F32)
        cs = pl.ds(pl.multiple_of(i * TILE, TILE), TILE)
        u_s[:, cs] = (a * jax.nn.sigmoid(a) * b).astype(BF16)
        start(t + nbuf)
        start(t + 1 + nbuf)

    @pl.loop(0, ny)
    def _(i):
        t = b_2 + kk * i
        slots = [ready(t + k) for k in range(kk)]
        acc = None
        for k in range(kk):
            r = jnp.dot(u_s[:, k * nk:(k + 1) * nk], wbuf[slots[k]], preferred_element_type=F32)
            acc = r if acc is None else acc + r
        cs = pl.ds(pl.multiple_of(i * TILE, TILE), TILE)
        xm_s[:, cs] = (xm_s[:, cs].astype(F32) + acc).astype(BF16)
        for k in range(kk):
            start(t + k + nbuf)

    y_at = half * rows if y_ref.shape[0] > rows else 0
    y_out = pltpu.make_async_copy(xm_s, y_ref.at[pl.ds(y_at, rows)], out_sem)
    y_out.start()

    if more:
        _norm_to(h_s, xm_s[...], g1_ref[...])
        per = TILE // width

        @pl.loop(0, nq)
        def _(i):
            t = b_q + 3 * i
            slots = [ready(t + m) for m in range(3)]
            for m in range(3):
                r = jnp.dot(h_s[...], wbuf[slots[m]], preferred_element_type=F32)
                for a in range(TILE // HEAD):
                    z = r[:, a * HEAD:(a + 1) * HEAD]
                    if m < 2:
                        z = z * cos_ref[...] + pltpu.roll(z, HEAD // 2, 1) * sin_ref[...]
                    lane = (a * HEAD) % width
                    nxt_ref[i * per + (a * HEAD) // width, m, :, lane:lane + HEAD] = z.astype(BF16)
            for m in range(3):
                start(t + m + nbuf)

    y_out.wait()
    if swap:
        keep().wait()
        for i in range(1, ncp):
            j = lax.rem(me + i, ncp)
            cross(j, me).wait_send()
            cross(j, j).wait_recv()


def _layer(layer, late, x, qkv, pre, other, y, tabs, w, more):
    g1, g2, wq, wk, wv, wo, w1, w3, w2 = w
    ncp, _, seg, width = qkv.shape
    half = int(late)
    d, ff = x.shape[1], w1.shape[2]
    anyspace = pl.BlockSpec(memory_space=pl.ANY)
    vmem = pl.BlockSpec(memory_space=pltpu.VMEM)
    nh = width // HEAD
    ins, specs = [x, qkv], [vmem, vmem]
    if late:
        ins.append(pre)
        specs.append(vmem)
    ins += [g2[layer:layer + 1], wo, w1, w3, w2]
    specs += [vmem] + [anyspace] * 4
    outs, ospecs = [jax.ShapeDtypeStruct((seg if more else 2 * seg, d), BF16)], [anyspace]
    block = jax.ShapeDtypeStruct(qkv.shape, BF16)
    if more:
        at = half * seg
        ins += [g1[layer + 1:layer + 2], tabs[0][at:at + seg], tabs[1][at:at + seg], wq, wk, wv]
        specs += [vmem] * 3 + [anyspace] * 3
        outs.append(block)
        ospecs.append(vmem)
    if other is not None:
        ins.append(other)
        specs.append(anyspace)
        outs.append(block)
        ospecs.append(anyspace)
    alias = {}
    if y is not None:
        alias = {len(ins): 0}
        ins.append(y)
        specs.append(anyspace)
    dma = pltpu.SemaphoreType.DMA
    scratch = [pltpu.VMEM((seg, d), BF16), pltpu.VMEM((RING, d, TILE), BF16), dma((RING,)),
               pltpu.VMEM((seg, d), BF16), pltpu.VMEM((seg, ff), BF16),
               pltpu.VMEM((ncp, seg, width), BF16), pltpu.VMEM((ncp, seg, width), BF16),
               pltpu.VMEM((nh, 2 * seg, 2 * HEAD), F32), pltpu.VMEM((nh, 2 * seg, HEAD), F32),
               dma((ncp,)), dma((ncp,)), dma]
    if other is not None:
        scratch += [dma((ncp,)), dma((ncp,))]
    flops = 2 * seg * d * (d + 3 * ff + (3 * d if more else 0))
    return pl.pallas_call(
        functools.partial(_layer_kernel, layer, late, more, other is not None, y is not None),
        out_shape=outs,
        in_specs=specs,
        out_specs=ospecs,
        scratch_shapes=scratch,
        input_output_aliases=alias,
        compiler_params=pltpu.CompilerParams(vmem_limit_bytes=VMEM_LIMIT, collective_id=2 * layer + half,
                                             has_side_effects=True),
        cost_estimate=pl.CostEstimate(flops=flops, bytes_accessed=flops // seg, transcendentals=0),
        name=f"layer_{layer}_{half}",
    )(*ins)


def solution(mesh):
    ncp = mesh.shape['cp']
    act = P(('req', 'cp'), None)
    cache = P(None, 'req', 'cp', None)

    def swap(a):
        return lax.all_to_all(a, 'cp', 0, 0, tiled=True)

    def body(x, pos, g1, g2, wq, wk, wv, wo, w1, w3, w2):
        w = (g1, g2, wq, wk, wv, wo, w1, w3, w2)
        layers = wq.shape[0]
        tabs = _tables(pos)
        xs = [x, x]
        qkv = [_dense(-1, i, x, None, tabs, w, ncp, False, True)[0] for i in range(2)]
        caches = None
        ra, other, y = swap(qkv[0]), qkv[1], None
        for l in range(layers):
            more = l + 1 < layers
            res = list(_layer(l, False, xs[0], ra, None, other, None, tabs, w, more))
            xa, rb = res[0], res[-1]
            nxt = res[1] if more else None
            res = list(_layer(l, True, xs[1], rb, ra, nxt, None if more else xa, tabs, w, more))
            caches = _cache(l, layers, ra, rb, caches)
            xs = [xa, res[0]]
            if more:
                other, ra = res[1], res[2]
        kc, vc = (a.reshape(layers, -1, wq.shape[2] // ncp // HEAD, HEAD) for a in caches)
        return xs[1], kc, vc

    return jax.shard_map(body, mesh=mesh, in_specs=(act, P(('req', 'cp'))) + (P(),) * 9,
                         out_specs=(act, cache, cache), check_vma=False)
```

```python
import functools
import math

import jax
import jax.numpy as jnp
from jax import lax
from jax.experimental import pallas as pl
from jax.experimental.pallas import tpu as pltpu
from jax.sharding import PartitionSpec as P

HEAD = 128
TILE = 512
NBUF = 9
RING = 14
F32 = jnp.float32
BF16 = jnp.bfloat16
VMEM_LIMIT = 60 * 1024 * 1024


def _tables(pos):
    half = HEAD // 2
    inv = 1.0 / (10000.0 ** (jnp.arange(half, dtype=F32) * (2.0 / HEAD)))
    ang = pos.astype(F32)[:, None] * inv
    c, s = jnp.cos(ang), jnp.sin(ang)
    return jnp.concatenate([c, c], axis=1), jnp.concatenate([-s, s], axis=1)


def _norm_to(dst, x, g):
    x32 = x.astype(F32)
    r = lax.rsqrt(jnp.mean(x32 * x32, axis=-1, keepdims=True) + 1e-5)
    dst[...] = (x32 * r * g.astype(F32)).astype(BF16)


def _first_kernel(x_ref, g_ref, cos_ref, sin_ref, wq, wk, wv, out_ref, late_ref,
                  h_s, wbuf, sems, qkv_s, send_sem, recv_sem):
    me = lax.axis_index('cp')
    ncp, _, seg, width = late_ref.shape
    nbuf = wbuf.shape[0]
    nq = wq.shape[2] // TILE
    per = TILE // width
    total = 2 * 3 * nq
    barrier = pltpu.get_barrier_semaphore()
    for i in range(1, ncp):
        pl.semaphore_signal(barrier, inc=1, device_id={'cp': lax.rem(me + i, ncp)},
                            device_id_type=pl.DeviceIdType.MESH)

    def group(i):
        return lax.rem(me // per + 1 + i, nq)

    def tile(w, i):
        return w.at[0, :, pl.ds(pl.multiple_of(group(i) * TILE, TILE), TILE)]

    def start(t, which):
        slot = t % nbuf if isinstance(t, int) else lax.rem(t, nbuf)
        i = t // 3
        pltpu.make_async_copy(tile((wq, wk, wv)[which], i), wbuf.at[slot], sems.at[slot]).start()

    def ready(t):
        slot = lax.rem(t, nbuf)
        pltpu.make_async_copy(tile(wq, 0), wbuf.at[slot], sems.at[slot]).wait()
        return slot

    def remote(j, slot):
        return pltpu.make_async_remote_copy(
            src_ref=qkv_s.at[j], dst_ref=out_ref.at[slot], send_sem=send_sem.at[j], recv_sem=recv_sem.at[slot],
            device_id={'cp': j}, device_id_type=pl.DeviceIdType.MESH)

    def local():
        return pltpu.make_async_copy(qkv_s.at[me], out_ref.at[me], recv_sem.at[me])

    for t in range(nbuf):
        start(t, t % 3)

    for half in range(2):
        at = half * seg
        dst = late_ref if half else qkv_s
        _norm_to(h_s, x_ref[at:at + seg, :], g_ref[...])

        @pl.loop(0, nq)
        def _(i):
            t = 3 * (half * nq + i)
            gi = group(i)
            slots = [ready(t + m) for m in range(3)]
            for m in range(3):
                r = jnp.dot(h_s[...], wbuf[slots[m]], preferred_element_type=F32)
                for a in range(TILE // HEAD):
                    z = r[:, a * HEAD:(a + 1) * HEAD]
                    if m < 2:
                        z = (z * cos_ref[at:at + seg, :]
                             + pltpu.roll(z, HEAD // 2, 1) * sin_ref[at:at + seg, :])
                    lane = (a * HEAD) % width
                    dst[gi * per + (a * HEAD) // width, m, :, lane:lane + HEAD] = z.astype(BF16)

            @pl.when(t + 2 + nbuf < total)
            def _():
                for m in range(3):
                    start(t + m + nbuf, (m + nbuf) % 3)

            if half == 0:
                @pl.when(i == 0)
                def _():
                    pl.semaphore_wait(barrier, ncp - 1)

                for a in range(per):
                    j = gi * per + a

                    @pl.when(j != me)
                    def _():
                        remote(j, me).start()

                    @pl.when(j == me)
                    def _():
                        local().start()

    local().wait()
    for i in range(1, ncp):
        j = lax.rem(me + i, ncp)
        remote(j, me).wait_send()
        remote(j, j).wait_recv()


def _first(x, tabs, w, ncp):
    g1, _, wq, wk, wv = w[:5]
    seg, d = x.shape[0] // 2, x.shape[1]
    width = wq.shape[2] // ncp
    anyspace = pl.BlockSpec(memory_space=pl.ANY)
    vmem = pl.BlockSpec(memory_space=pltpu.VMEM)
    block = jax.ShapeDtypeStruct((ncp, 3, seg, width), BF16)
    dma = pltpu.SemaphoreType.DMA
    flops = 12 * seg * d * wq.shape[2]
    return pl.pallas_call(
        _first_kernel,
        out_shape=[block, block],
        in_specs=[vmem] * 4 + [anyspace] * 3,
        out_specs=[anyspace, vmem],
        scratch_shapes=[pltpu.VMEM((seg, d), BF16), pltpu.VMEM((NBUF, d, TILE), BF16), dma((NBUF,)),
                        pltpu.VMEM(block.shape, BF16), dma((ncp,)), dma((ncp,))],
        compiler_params=pltpu.CompilerParams(vmem_limit_bytes=VMEM_LIMIT, collective_id=2 * wq.shape[0],
                                             has_side_effects=True),
        cost_estimate=pl.CostEstimate(flops=flops, bytes_accessed=flops // seg, transcendentals=0),
        name="first",
    )(x, g1[:1], tabs[0], tabs[1], wq, wk, wv)


def _cache_kernel(first, ka_ref, va_ref, kb_ref, vb_ref, *refs):
    kc_ref, vc_ref, il_s = refs if first else refs[2:]
    n = pl.program_id(0)
    half = pl.num_programs(0) // 2
    seg, width = ka_ref.shape[2], ka_ref.shape[3]
    nh = width // HEAD

    def write(pair, order):
        for which, out in ((1, kc_ref), (2, vc_ref)):
            for i in range(4):
                src = pair[which - 1][order[i], 0]
                for h in range(nh):
                    il_s[which - 1, pl.ds(i * seg * nh + h, seg, stride=nh), :] = (
                        src[:, h * HEAD:(h + 1) * HEAD].astype(F32))
            out[0] = il_s[which - 1].astype(BF16)

    @pl.when(n < half)
    def _():
        write((ka_ref, va_ref), (0, 1, 2, 3))

    @pl.when(n >= half)
    def _():
        write((kb_ref, vb_ref), (3, 2, 1, 0))


def _cache(layer, layers, ra, rb, caches):
    ncp, _, seg, width = ra.shape
    nh = width // HEAD
    nq = ncp // 4
    rows = 4 * seg * nh
    ins = [ra, ra, rb, rb]
    block = (4, 1, seg, width)
    specs = [pl.BlockSpec(block, lambda n, m=m: (jnp.minimum(n, nq - 1), m, 0, 0)) for m in (1, 2)]
    specs += [pl.BlockSpec(block, lambda n, m=m: (jnp.minimum(2 * nq - 1 - n, nq - 1), m, 0, 0)) for m in (1, 2)]
    alias = {}
    if caches is not None:
        alias = {4: 0, 5: 1}
        ins += list(caches)
        specs += [pl.BlockSpec(memory_space=pl.ANY)] * 2
    cache = jax.ShapeDtypeStruct((layers, 2 * ncp * seg * nh, HEAD), BF16)
    spec = pl.BlockSpec((1, rows, HEAD), lambda n: (layer, n, 0))
    return pl.pallas_call(
        functools.partial(_cache_kernel, caches is None),
        grid=(2 * nq,),
        out_shape=[cache, cache],
        in_specs=specs,
        out_specs=[spec, spec],
        scratch_shapes=[pltpu.VMEM((2, rows, HEAD), F32)],
        input_output_aliases=alias,
        compiler_params=pltpu.CompilerParams(dimension_semantics=("arbitrary",)),
        cost_estimate=pl.CostEstimate(flops=4 * 10 ** 9, bytes_accessed=10 * ncp * seg * width * 2,
                                      transcendentals=0),
        name=f"cache_{layer}",
    )(*ins)


def _layer_kernel(layer, late, more, swap, joined, *refs):
    refs = list(refs)
    x_ref, qkv_ref = refs[:2]
    refs = refs[2:]
    pre_ref = refs.pop(0) if late else None
    g2_ref, wo, w1, w3, w2 = refs[:5]
    refs = refs[5:]
    if more:
        g1_ref, cos_ref, sin_ref, wq, wk, wv = refs[:6]
        refs = refs[6:]
    if swap:
        ex_in = refs.pop(0)
    if joined:
        refs.pop(0)
    y_ref = refs.pop(0)
    if more:
        nxt_ref = refs.pop(0)
    if swap:
        ex_out = refs.pop(0)
    h_s, wbuf, sems, xm_s, u_s, o_s, o_r, acc_s, m_s, send_sem, recv_sem, out_sem = refs[:12]
    if swap:
        xs_sem, xr_sem = refs[12:]
    nbuf = wbuf.shape[0]
    half = int(late)
    rows, d = h_s.shape
    nk = wbuf.shape[1]
    ncp, _, seg, width = qkv_ref.shape
    npair = ncp // 2
    nh = width // HEAD
    bq = 2 * seg
    scale = HEAD ** -0.5 * math.log2(math.e)
    me = lax.axis_index('cp')
    barrier = pltpu.get_barrier_semaphore()
    for i in range(1, ncp):
        pl.semaphore_signal(barrier, inc=1, device_id={'cp': lax.rem(me + i, ncp)},
                            device_id_type=pl.DeviceIdType.MESH)

    def col(i):
        return pl.ds(i * TILE, TILE)

    no, nf = wo.shape[2] // TILE, w1.shape[2] // TILE
    kk, ny = w2.shape[1] // nk, w2.shape[2] // TILE
    b_o, b_1, b_2 = 0, no, no + 2 * nf
    b_q = b_2 + ny * kk
    segs = [(b_o, no, lambda i: [wo.at[layer, :, col(i)]]),
            (b_1, 2 * nf, lambda i: [w1.at[layer, :, col(i // 2)], w3.at[layer, :, col(i // 2)]]),
            (b_2, ny * kk, lambda i: [w2.at[layer, pl.ds((i % kk) * nk, nk), col(i // kk)]])]
    if more:
        nq = wq.shape[2] // TILE
        segs.append((b_q, 3 * nq, lambda i: [w.at[layer + 1, :, col(i // 3)] for w in (wq, wk, wv)]))

    def start(t):
        slot = t % nbuf if isinstance(t, int) else lax.rem(t, nbuf)
        for first, n, srcs in segs:
            if isinstance(t, int):
                if first <= t < first + n:
                    lst = srcs(t - first)
                    pltpu.make_async_copy(lst[(t - first) % len(lst)], wbuf.at[slot], sems.at[slot]).start()
                continue
            i = t - first
            lst = srcs(i)
            for which, src in enumerate(lst):
                cond = (t >= first) & (t < first + n)
                if len(lst) > 1:
                    cond = cond & (lax.rem(i, len(lst)) == which)

                @pl.when(cond)
                def _(src=src):
                    pltpu.make_async_copy(src, wbuf.at[slot], sems.at[slot]).start()

    def ready(t):
        slot = lax.rem(t, nbuf)
        pltpu.make_async_copy(wo.at[layer, :, col(0)], wbuf.at[slot], sems.at[slot]).wait()
        return slot

    for t in range(nbuf):
        start(t)

    ones = jnp.ones((bq, HEAD), BF16)

    def block(ref, j, which, h):
        return ref[pl.ds(2 * j, 2), which, :, h * HEAD:(h + 1) * HEAD].reshape(bq, HEAD)

    def wide(a, n):
        return jnp.concatenate([a] * n, axis=1)

    def remote(j, slot):
        return pltpu.make_async_remote_copy(
            src_ref=o_s.at[j], dst_ref=o_r.at[slot], send_sem=send_sem.at[j], recv_sem=recv_sem.at[slot],
            device_id={'cp': j}, device_id_type=pl.DeviceIdType.MESH)

    def local():
        return pltpu.make_async_copy(o_s.at[me], o_r.at[me], recv_sem.at[me])

    def cross(j, slot):
        return pltpu.make_async_remote_copy(
            src_ref=ex_in.at[j], dst_ref=ex_out.at[slot], send_sem=xs_sem.at[j], recv_sem=xr_sem.at[slot],
            device_id={'cp': j}, device_id_type=pl.DeviceIdType.MESH)

    def keep():
        return pltpu.make_async_copy(ex_in.at[me], ex_out.at[me], xr_sem.at[me])

    def cross_chip(k):
        for a in range(2):
            cross(2 * lax.rem(me // 2 + k, npair) + a, me).start()

    @pl.loop(0, npair)
    def _(step):
        p = lax.rem(me // 2 + 1 + step, npair)

        def scores(ref, j, h):
            return lax.dot_general(block(qkv_ref, p, 0, h), block(ref, j, 1, h), (((1,), (1,)), ((), ())),
                                   preferred_element_type=F32)

        r = lax.broadcasted_iota(jnp.int32, (bq, bq), 0)
        c = lax.broadcasted_iota(jnp.int32, (bq, bq), 1)
        if late:
            r = jnp.where(r < seg, r + seg, r - seg)
            c = jnp.where(c < seg, c + seg, c - seg)
        mask = c <= r
        for h in range(nh):
            s = jnp.where(mask, scores(qkv_ref, p, h), -jnp.inf)
            m = jnp.broadcast_to(jnp.max(s, axis=1, keepdims=True), (bq, HEAD))
            pr = jnp.exp2((s - wide(m, bq // HEAD)) * scale).astype(BF16)
            v = jnp.concatenate([block(qkv_ref, p, 2, h), ones], axis=1)
            acc_s[h] = jnp.dot(pr, v, preferred_element_type=F32)
            m_s[h] = m

        def full(ref, j):
            ss = [scores(ref, j, h) for h in range(nh)]
            for h in range(nh):
                s = ss[h]
                old = m_s[h]
                m = jnp.maximum(old, jnp.broadcast_to(jnp.max(s, axis=1, keepdims=True), (bq, HEAD)))
                pr = jnp.exp2((s - wide(m, bq // HEAD)) * scale).astype(BF16)
                v = jnp.concatenate([block(ref, j, 2, h), ones], axis=1)
                alpha = jnp.exp2((old - m) * scale)
                acc_s[h] = acc_s[h] * wide(alpha, 2) + jnp.dot(pr, v, preferred_element_type=F32)
                m_s[h] = m

        if late:
            @pl.loop(0, npair)
            def _(j):
                full(pre_ref, j)

            @pl.loop(p + 1, npair)
            def _(j):
                full(qkv_ref, j)
        else:
            @pl.loop(0, p)
            def _(j):
                full(qkv_ref, j)

        for h in range(nh):
            o = (acc_s[h, :, :HEAD] / acc_s[h, :, HEAD:]).astype(BF16)
            o_s[pl.ds(2 * p, 2), :, h * HEAD:(h + 1) * HEAD] = o.reshape(2, seg, HEAD)

        @pl.when(step == 0)
        def _():
            pl.semaphore_wait(barrier, ncp - 1)

        for a in range(2):
            j = 2 * p + a

            @pl.when(j != me)
            def _():
                remote(j, me).start()

            @pl.when(j == me)
            def _():
                local().start()

        if swap:
            @pl.when(step == 1)
            def _():
                cross_chip(1)

            @pl.when(step == npair - 2)
            def _():
                cross_chip(npair - 1)

    if swap:
        for k in range(2, npair - 1):
            cross_chip(k)
        cross(me + 1 - 2 * lax.rem(me, 2), me).start()
        keep().start()

    local().wait()
    for i in range(1, ncp):
        j = lax.rem(me + i, ncp)
        remote(j, me).wait_send()
        remote(j, j).wait_recv()

    for j in range(ncp):
        h_s[:, j * width:(j + 1) * width] = o_r[j]
    x_at = half * rows if x_ref.shape[0] > rows else 0

    @pl.loop(0, no)
    def _(i):
        t = b_o + i
        slot = ready(t)
        cs = pl.ds(pl.multiple_of(i * TILE, TILE), TILE)
        r = jnp.dot(h_s[...], wbuf[slot], preferred_element_type=F32)
        xm_s[:, cs] = (x_ref[x_at:x_at + rows, cs].astype(F32) + r).astype(BF16)
        start(t + nbuf)

    _norm_to(h_s, xm_s[...], g2_ref[...])

    @pl.loop(0, nf)
    def _(i):
        t = b_1 + 2 * i
        s1 = ready(t)
        s3 = ready(t + 1)
        a = jnp.dot(h_s[...], wbuf[s1], preferred_element_type=F32)
        b = jnp.dot(h_s[...], wbuf[s3], preferred_element_type=F32)
        cs = pl.ds(pl.multiple_of(i * TILE, TILE), TILE)
        u_s[:, cs] = (a * jax.nn.sigmoid(a) * b).astype(BF16)
        start(t + nbuf)
        start(t + 1 + nbuf)

    @pl.loop(0, ny)
    def _(i):
        t = b_2 + kk * i
        slots = [ready(t + k) for k in range(kk)]
        acc = None
        for k in range(kk):
            r = jnp.dot(u_s[:, k * nk:(k + 1) * nk], wbuf[slots[k]], preferred_element_type=F32)
            acc = r if acc is None else acc + r
        cs = pl.ds(pl.multiple_of(i * TILE, TILE), TILE)
        xm_s[:, cs] = (xm_s[:, cs].astype(F32) + acc).astype(BF16)
        for k in range(kk):
            start(t + k + nbuf)

    y_at = half * rows if y_ref.shape[0] > rows else 0
    y_out = pltpu.make_async_copy(xm_s, y_ref.at[pl.ds(y_at, rows)], out_sem)
    y_out.start()

    if more:
        _norm_to(h_s, xm_s[...], g1_ref[...])
        per = TILE // width

        @pl.loop(0, nq)
        def _(i):
            t = b_q + 3 * i
            slots = [ready(t + m) for m in range(3)]
            for m in range(3):
                r = jnp.dot(h_s[...], wbuf[slots[m]], preferred_element_type=F32)
                for a in range(TILE // HEAD):
                    z = r[:, a * HEAD:(a + 1) * HEAD]
                    if m < 2:
                        z = z * cos_ref[...] + pltpu.roll(z, HEAD // 2, 1) * sin_ref[...]
                    lane = (a * HEAD) % width
                    nxt_ref[i * per + (a * HEAD) // width, m, :, lane:lane + HEAD] = z.astype(BF16)
            for m in range(3):
                start(t + m + nbuf)

    y_out.wait()
    if swap:
        keep().wait()
        for i in range(1, ncp):
            j = lax.rem(me + i, ncp)
            cross(j, me).wait_send()
            cross(j, j).wait_recv()


def _layer(layer, late, x, qkv, pre, other, y, tabs, w, more):
    g1, g2, wq, wk, wv, wo, w1, w3, w2 = w
    ncp, _, seg, width = qkv.shape
    half = int(late)
    d, ff = x.shape[1], w1.shape[2]
    anyspace = pl.BlockSpec(memory_space=pl.ANY)
    vmem = pl.BlockSpec(memory_space=pltpu.VMEM)
    nh = width // HEAD
    ins, specs = [x, qkv], [vmem, vmem]
    if late:
        ins.append(pre)
        specs.append(vmem)
    ins += [g2[layer:layer + 1], wo, w1, w3, w2]
    specs += [vmem] + [anyspace] * 4
    outs, ospecs = [jax.ShapeDtypeStruct((seg if more else 2 * seg, d), BF16)], [anyspace]
    block = jax.ShapeDtypeStruct(qkv.shape, BF16)
    if more:
        at = half * seg
        ins += [g1[layer + 1:layer + 2], tabs[0][at:at + seg], tabs[1][at:at + seg], wq, wk, wv]
        specs += [vmem] * 3 + [anyspace] * 3
        outs.append(block)
        ospecs.append(vmem)
    if other is not None:
        ins.append(other)
        specs.append(anyspace)
        outs.append(block)
        ospecs.append(anyspace)
    alias = {}
    if y is not None:
        alias = {len(ins): 0}
        ins.append(y)
        specs.append(anyspace)
    dma = pltpu.SemaphoreType.DMA
    scratch = [pltpu.VMEM((seg, d), BF16), pltpu.VMEM((RING, d, TILE), BF16), dma((RING,)),
               pltpu.VMEM((seg, d), BF16), pltpu.VMEM((seg, ff), BF16),
               pltpu.VMEM((ncp, seg, width), BF16), pltpu.VMEM((ncp, seg, width), BF16),
               pltpu.VMEM((nh, 2 * seg, 2 * HEAD), F32), pltpu.VMEM((nh, 2 * seg, HEAD), F32),
               dma((ncp,)), dma((ncp,)), dma]
    if other is not None:
        scratch += [dma((ncp,)), dma((ncp,))]
    flops = 2 * seg * d * (d + 3 * ff + (3 * d if more else 0))
    return pl.pallas_call(
        functools.partial(_layer_kernel, layer, late, more, other is not None, y is not None),
        out_shape=outs,
        in_specs=specs,
        out_specs=ospecs,
        scratch_shapes=scratch,
        input_output_aliases=alias,
        compiler_params=pltpu.CompilerParams(vmem_limit_bytes=VMEM_LIMIT, collective_id=2 * layer + half,
                                             has_side_effects=True),
        cost_estimate=pl.CostEstimate(flops=flops, bytes_accessed=flops // seg, transcendentals=0),
        name=f"layer_{layer}_{half}",
    )(*ins)


def solution(mesh):
    ncp = mesh.shape['cp']
    act = P(('req', 'cp'), None)
    cache = P(None, 'req', 'cp', None)

    def body(x, pos, g1, g2, wq, wk, wv, wo, w1, w3, w2):
        w = (g1, g2, wq, wk, wv, wo, w1, w3, w2)
        layers = wq.shape[0]
        tabs = _tables(pos)
        xs = [x, x]
        caches = None
        ra, other = _first(x, tabs, w, ncp)
        for l in range(layers):
            more = l + 1 < layers
            res = list(_layer(l, False, xs[0], ra, None, other, None, tabs, w, more))
            xa, rb = res[0], res[-1]
            nxt = res[1] if more else None
            res = list(_layer(l, True, xs[1], rb, ra, nxt, None if more else xa, tabs, w, more))
            caches = _cache(l, layers, ra, rb, caches)
            xs = [xa, res[0]]
            if more:
                other, ra = res[1], res[2]
        kc, vc = (a.reshape(layers, -1, wq.shape[2] // ncp // HEAD, HEAD) for a in caches)
        return xs[1], kc, vc

    return jax.shard_map(body, mesh=mesh, in_specs=(act, P(('req', 'cp'))) + (P(),) * 9,
                         out_specs=(act, cache, cache), check_vma=False)
```
